32 devices in a mesh: gx: 4 (over y, x), gy: 8 (over z, core).
Axes of the slice: x: 2, y: 2, z: 4, core: 2. Of those that a mesh axis runs over, the one named last changes fastest.
Arguments:
- velocity: float32 [3, 128, 64, 128], P(None, 'gx', 'gy'), may hold values from -6 to 6
- stress: float32 [6, 128, 64, 128], P(None, 'gx', 'gy'), may hold values from -6 to 6
- lame_first: float32 [128, 64, 128], P('gx', 'gy'), may hold values from 0.5 to 2
- modulus: float32 [128, 64, 128], P('gx', 'gy'), may hold values from 0.5 to 2
- buoyancy: float32 [128, 64, 128], P('gx', 'gy'), may hold values from 0.5 to 2
- zone: int32 [128, 64, 128], P('gx', 'gy'), may hold values from 0 to 7
- eligible: int32 [128, 64, 128], P('gx', 'gy'), may hold values 0 or 1
- cohesion: float32 [8], replicated, may hold values from 0.2 to 2
- friction: float32 [8], replicated, may hold values from 0.1 to 0.6
- source_cell: int32 [16], replicated, may hold values from 0 to 1048575
- source_moment: float32 [6, 16], replicated, may hold values from -15 to 15
Outputs:
- velocity_out: float32 [3, 128, 64, 128], P(None, 'gx', 'gy')
- stress_out: float32 [6, 128, 64, 128], P(None, 'gx', 'gy')
The draws below stay inside these ranges and needn't reach their ends.
All inputs are finite; a program needn't handle non-finite values. No bound on the sum of `eligible` on one device may be relied on, other than what follows from the above.
Results may differ from the reference program's by a relative error of at most 0.00011.
Values sent between devices are 32-bit elements; how exact they have to be, the bound alone decides.
A program may use at most 64 MiB of HBM per device.

```python
import math
import jax
import jax.numpy as jnp
from jax import lax

NZ = 128
STEPS = 2
NZONES = 8
NSRC = 16
NX = 128
NY = 64


def with_ends(values, stream_key, low, largest):
    longest = values.shape.index(max(values.shape))
    spots = []
    for shift in (0, 1):
        where = [jax.random.randint(jax.random.fold_in(stream_key, axis), (), 0, length) for axis, length in enumerate(values.shape)]
        where[longest] = (where[longest] + shift) % values.shape[longest]
        spots.append(tuple(where))
    return values.at[spots[0]].set(low).at[spots[1]].set(largest)


def levels(stream_key, shape, cuts, smallest, high):
    def one(position, parts):
        steps = jax.random.uniform(jax.random.fold_in(jax.random.fold_in(stream_key, 6), position), (parts,), jnp.float32, smallest / len(cuts), high / len(cuts))
        return jnp.repeat(jnp.exp(steps), shape[position] // parts).reshape((-1,) + (1,) * (len(shape) - position - 1))

    level = one(*cuts[0])
    for cut in cuts[1:]:
        level = level * one(*cut)
    return level


def centred(key, extent, deviation, most, pieces=(), dtype=jnp.bfloat16):
    array = jax.random.normal(key, extent, jnp.float32) * deviation
    if len(pieces) > 0:
        array = levels(key, extent, pieces, -0.22, 0.18) * array
    return jnp.clip(array, min=-most, max=most).astype(dtype)


def setup_inputs(seed: int = 0) -> dict:
    seeds = jax.random.split(jax.random.key(seed), 12)
    return {
        "velocity": centred(seeds[0], (3, NX, NY, NZ), 1.0, 6.0, ((1, 4), (2, 8)), jnp.float32),
        "stress": centred(seeds[1], (6, NX, NY, NZ), 1.0, 6.0, ((1, 4), (2, 8)), jnp.float32),
        "lame_first": jnp.clip(jnp.exp(math.log(2.0) - 1.3862944 * jax.random.uniform(seeds[2], (NX, NY, NZ), jnp.float32) ** levels(seeds[2], (NX, NY, NZ), ((0, 4), (1, 8)), -0.2, 0.2)), 0.5, 2.0),
        "modulus": jnp.clip(jnp.exp(math.log(2.0) - 1.3862944 * jax.random.uniform(seeds[3], (NX, NY, NZ), jnp.float32) ** levels(seeds[3], (NX, NY, NZ), ((0, 4), (1, 8)), -0.2, 0.2)), 0.5, 2.0),
        "buoyancy": jnp.clip(jnp.exp(math.log(2.0) - 1.3862944 * jax.random.uniform(seeds[4], (NX, NY, NZ), jnp.float32) ** levels(seeds[4], (NX, NY, NZ), ((0, 4), (1, 8)), -0.2, 0.2)), 0.5, 2.0),
        "zone": with_ends(jax.random.randint(seeds[5], (NX, NY, NZ), 0, NZONES), jax.random.fold_in(seeds[5], 1), 0, NZONES - 1).astype(jnp.int32),
        "eligible": with_ends((jax.random.randint(seeds[6], (NX, NY, NZ), 0, 2) < 1).astype(jnp.int32), jax.random.fold_in(seeds[6], 1), 0, 1),
        "cohesion": jnp.clip(jnp.exp(jax.random.uniform(seeds[7], (NZONES,), jnp.float32, math.log(0.2), math.log(2.0))), 0.2, 2.0),
        "friction": jnp.clip(jax.random.uniform(seeds[8], (NZONES,), jnp.float32, 0.1, 0.6), 0.1, 0.6),
        "source_cell": with_ends(jax.random.randint(seeds[9], (NSRC,), 0, NX * NY * NZ), jax.random.fold_in(seeds[9], 1), 0, (NX * NY * NZ) - 1).astype(jnp.int32),
        "source_moment": centred(seeds[10], (6, NSRC), 3.0, 15.0, (), jnp.float32),
    }


time_step = 0.1
near_weight = 9.0 / 8.0
far_weight = 1.0 / 24.0
shear_floor = 0.25

def crop(padded, axis, offset):
    result = padded
    for dim in range(3):
        begin = offset if dim == axis else 2
        length = padded.shape[dim] - 4
        result = lax.slice_in_dim(result, begin, begin + length, axis=dim)
    return result

def derivative(padded, axis, forward):
    if forward:
        return near_weight * (crop(padded, axis, 3) - crop(padded, axis, 2)) - far_weight * (crop(padded, axis, 4) - crop(padded, axis, 1))
    return near_weight * (crop(padded, axis, 2) - crop(padded, axis, 1)) - far_weight * (crop(padded, axis, 3) - crop(padded, axis, 0))

def velocity_update(stress_pad, velocity, buoyancy):
    force_x = derivative(stress_pad[0], 0, True) + derivative(stress_pad[3], 1, False) + derivative(stress_pad[4], 2, False)
    force_y = derivative(stress_pad[3], 0, False) + derivative(stress_pad[1], 1, True) + derivative(stress_pad[5], 2, False)
    force_z = derivative(stress_pad[4], 0, False) + derivative(stress_pad[5], 1, False) + derivative(stress_pad[2], 2, True)
    forces = jnp.stack([force_x, force_y, force_z])
    return velocity + time_step * buoyancy[None] * forces

def stress_update(flow_pad, stress, lame_first, modulus):
    strain_x = derivative(flow_pad[0], 0, False)
    strain_y = derivative(flow_pad[1], 1, False)
    strain_z = derivative(flow_pad[2], 2, False)
    dilation = strain_x + strain_y + strain_z
    shear_xy = derivative(flow_pad[0], 1, True) + derivative(flow_pad[1], 0, True)
    shear_xz = derivative(flow_pad[0], 2, True) + derivative(flow_pad[2], 0, True)
    shear_yz = derivative(flow_pad[1], 2, True) + derivative(flow_pad[2], 1, True)
    rates = jnp.stack([lame_first * dilation + 2.0 * modulus * strain_x, lame_first * dilation + 2.0 * modulus * strain_y, lame_first * dilation + 2.0 * modulus * strain_z, modulus * shear_xy, modulus * shear_xz, modulus * shear_yz])
    return stress + time_step * rates

def plastic(stress, cell_cohesion, cell_friction, eligible):
    pressure = (stress[0] + stress[1] + stress[2]) / 3.0
    dev_x = stress[0] - pressure
    dev_y = stress[1] - pressure
    dev_z = stress[2] - pressure
    second = 0.5 * (dev_x * dev_x + dev_y * dev_y + dev_z * dev_z) + stress[3] * stress[3] + stress[4] * stress[4] + stress[5] * stress[5]
    strength = jnp.maximum(cell_cohesion * jnp.sqrt(1.0 - cell_friction * cell_friction) - pressure * cell_friction, 0.0)
    ratio = jnp.minimum(1.0, strength / jnp.maximum(jnp.sqrt(second), shear_floor))
    factor = jnp.where(eligible == 1, ratio, 1.0)
    return jnp.stack([pressure + factor * dev_x, pressure + factor * dev_y, pressure + factor * dev_z, factor * stress[3], factor * stress[4], factor * stress[5]])

def pad_space(field, width):
    return jnp.pad(field, ((0, 0), (width, width), (width, width), (width, width)))

def reference(velocity, stress, lame_first, modulus, buoyancy, zone, eligible, cohesion, friction, source_cell, source_moment):
    cell_cohesion = cohesion[zone]
    cell_friction = friction[zone]
    plane = NY * NZ
    src_x = (source_cell // plane).astype(jnp.int32)
    src_y = (source_cell // NZ % NY).astype(jnp.int32)
    src_z = (source_cell % NZ).astype(jnp.int32)
    injection = jnp.zeros_like(stress).at[:, src_x, src_y, src_z].add(time_step * source_moment)
    for step in range(STEPS):
        velocity = velocity_update(pad_space(stress, 2), velocity, buoyancy)
        stress = stress_update(pad_space(velocity, 2), stress, lame_first, modulus)
        stress = stress + injection
        stress = plastic(stress, cell_cohesion, cell_friction, eligible)
    return (velocity, stress)
```

```python
import functools

import jax
import jax.numpy as jnp
from jax import lax
from jax.experimental import pallas as pl
from jax.experimental.pallas import tpu as pltpu
from jax.sharding import PartitionSpec as P

STEPS = 2
time_step = 0.1
shear_floor = 0.25
MESH = pl.DeviceIdType.MESH
CH = 8
R = 16
UNROLL = 2

STRESS_X = ((0, 1, 2), (3, 2, 1), (4, 2, 1))
STRESS_Y = ((3, 2, 1), (1, 1, 2), (5, 2, 1))
FLOW_X = ((0, 2, 1), (1, 1, 2), (2, 1, 2))
FLOW_Y = ((0, 1, 2), (1, 2, 1), (2, 1, 2))
SPEC = {"s": (STRESS_X, STRESS_Y), "v": (FLOW_X, FLOW_Y)}


def kernel(
    nx,
    ny,
    vel_hbm, str_hbm, lam_hbm, mod_hbm, buo_hbm, zone_hbm, elig_hbm,
    coh_ref, fri_ref, cell_ref, moment_ref,
    vout_hbm, sout_hbm,
    stage, vel, lam, mod, buo, zone, elig, inj, cc, cf, sout,
    xb, yb, zb, pack_up, pack_dn, recv_up, recv_dn,
    load_sem, store_sem, xsend, xrecv, ysend, yrecv,
):
    rows_x = lam.shape[0]
    rows_y = lam.shape[1]
    depth = lam.shape[2]
    chunks = rows_x // CH
    block = R * (rows_x + 1)
    phases = 2 * STEPS
    ix = lax.axis_index("gx")
    iy = lax.axis_index("gy")
    x_lo, x_hi, y_lo, y_hi = ix > 0, ix < nx - 1, iy > 0, iy < ny - 1

    loads = []

    def load(src, dst):
        copy = pltpu.make_async_copy(src, dst, load_sem.at[len(loads)])
        copy.start()
        loads.append(copy)

    for slot, (comp, _, _) in enumerate(STRESS_X):
        load(str_hbm.at[comp], xb.at[0, slot, pl.ds(2, rows_x)])
    load(str_hbm.at[1], stage.at[0])
    load(str_hbm.at[5], stage.at[1])
    load(str_hbm.at[2], zb.at[0])
    load(zone_hbm, zone)
    load(elig_hbm, elig)
    load(vel_hbm, vel)
    load(buo_hbm, buo)
    load(lam_hbm, lam)
    load(mod_hbm, mod)

    barrier = pltpu.get_barrier_semaphore()
    sides = (
        (x_lo, (ix - 1, iy)),
        (x_hi, (ix + 1, iy)),
        (y_lo, (ix, iy - 1)),
        (y_hi, (ix, iy + 1)),
    )
    for there, target in sides:

        @pl.when(there)
        def _():
            pl.semaphore_signal(barrier, inc=1, device_id=target, device_id_type=MESH)

    zero = jnp.zeros((rows_y, depth), jnp.float32)

    @pl.when(jnp.logical_not(x_lo))
    def _():
        for p in range(phases):
            for slot in range(3):
                for layer in (0, 1):
                    xb[p, slot, layer] = zero

    @pl.when(jnp.logical_not(x_hi))
    def _():
        for p in range(phases):
            for slot in range(3):
                for layer in (rows_x + 2, rows_x + 3):
                    xb[p, slot, layer] = zero

    @pl.when(jnp.logical_not(y_lo))
    def _():
        for p in range(phases):
            for c in range(chunks):
                recv_up[p, c] = jnp.zeros(recv_up.shape[2:], jnp.float32)

    @pl.when(jnp.logical_not(y_hi))
    def _():
        for p in range(phases):
            for c in range(chunks):
                recv_dn[p, c] = jnp.zeros(recv_dn.shape[2:], jnp.float32)

    def x_copy(p, slot, up):
        comp, low, high = SPEC["sv"[p % 2]][0][slot]
        if up:
            src = xb.at[p, slot, pl.ds(rows_x + 2 - low, low)]
            dst = xb.at[p, slot, pl.ds(2 - low, low)]
            target = (ix + 1, iy)
        else:
            src = xb.at[p, slot, pl.ds(2, high)]
            dst = xb.at[p, slot, pl.ds(rows_x + 2, high)]
            target = (ix - 1, iy)
        way = 0 if up else 1
        return pltpu.make_async_remote_copy(
            src_ref=src,
            dst_ref=dst,
            send_sem=xsend.at[p, way, slot],
            recv_sem=xrecv.at[p, way, slot],
            device_id=target,
            device_id_type=MESH,
        )

    def y_layers(p):
        spec = SPEC["sv"[p % 2]][1]
        up = [(slot, rows_y - low + i, i - low) for slot, (_, low, _) in enumerate(spec) for i in range(low)]
        dn = [(slot, i, rows_y + i) for slot, (_, _, high) in enumerate(spec) for i in range(high)]
        return up, dn

    def y_copy(p, c, up):
        rows = CH * len(y_layers(p)[0 if up else 1])
        packed, recv = (pack_up, recv_up) if up else (pack_dn, recv_dn)
        way = 0 if up else 1
        return pltpu.make_async_remote_copy(
            src_ref=packed.at[p, c, pl.ds(0, rows)],
            dst_ref=recv.at[p, c, pl.ds(0, rows)],
            send_sem=ysend.at[p, way, c],
            recv_sem=yrecv.at[p, way, c],
            device_id=(ix, iy + 1) if up else (ix, iy - 1),
            device_id_type=MESH,
        )

    def send_x(p, up):
        @pl.when(x_hi if up else x_lo)
        def _():
            for slot in range(3):
                x_copy(p, slot, up).start()

    def take_x(p, up):
        @pl.when(x_lo if up else x_hi)
        def _():
            for slot in range(3):
                x_copy(p, slot, up).wait_recv()

    def ybase(p, slot, x):
        return (p * 3 + slot) * block + R * (x + 1)

    def send_y(p, c):
        up, dn = y_layers(p)
        for layers, packed in ((up, pack_up), (dn, pack_dn)):
            for i, (slot, row, _) in enumerate(layers):
                start = ybase(p, slot, c * CH) + row
                packed[p, c, pl.ds(i * CH, CH), :] = yb[pl.ds(start, CH, stride=R), :]
        for there, way in ((y_hi, True), (y_lo, False)):

            @pl.when(there)
            def _():
                y_copy(p, c, way).start()

    def take_y(p, c):
        for there, way in ((y_lo, True), (y_hi, False)):

            @pl.when(there)
            def _():
                y_copy(p, c, way).wait_recv()

        up, dn = y_layers(p)
        for layers, recv in ((up, recv_up), (dn, recv_dn)):
            for i, (slot, _, row) in enumerate(layers):
                start = ybase(p, slot, c * CH) + row
                yb[pl.ds(start, CH, stride=R), :] = recv[p, c, pl.ds(i * CH, CH), :]

    order = [0] + ([chunks - 1] if chunks > 1 else []) + list(range(1, chunks - 1))

    for copy in loads[:5]:
        copy.wait()

    def fill_y(c):
        def fill(i, carry):
            x = c * CH + i
            for slot, source in enumerate((None, 0, 1)):
                value = xb[0, 1, x + 2] if source is None else stage[source, x]
                yb[pl.ds(pl.multiple_of(ybase(0, slot, x), 8), rows_y), :] = value
            return carry

        lax.fori_loop(0, CH, fill, 0, unroll=True)

    heard = sum(there.astype(jnp.int32) for there, _ in sides)
    pl.semaphore_wait(barrier, heard)
    send_x(0, True)
    send_x(0, False)
    for c in order:
        fill_y(c)
        send_y(0, c)

    cell = cell_ref[...]
    bits = depth.bit_length() - 1
    assert depth == 1 << bits
    plane_row = cell >> bits
    cell_z = cell & (depth - 1)
    row = lax.broadcasted_iota(jnp.int32, (rows_x * rows_y, cell.shape[1]), 0)
    row_bits = rows_y.bit_length() - 1
    assert rows_y == 1 << row_bits
    row = (ix * rows_x + (row >> row_bits)) * (ny * rows_y) + iy * rows_y + (row & (rows_y - 1))
    match = row == plane_row
    at_z = (lax.broadcasted_iota(jnp.int32, (depth, cell.shape[1]), 0) == cell_z).astype(jnp.float32)
    for comp in range(6):
        moment = time_step * moment_ref[pl.ds(comp, 1), :]
        value = lax.dot_general(
            jnp.where(match, moment, 0.0),
            at_z,
            (((1,), (1,)), ((), ())),
            precision=lax.Precision.HIGHEST,
            preferred_element_type=jnp.float32,
        )
        inj[comp] = value.reshape(rows_x, rows_y, depth)

    for copy in loads[6:8]:
        copy.wait()
    frictions, cohesions = [], []
    for which in range(coh_ref.shape[0]):
        f = jnp.full((rows_y, depth), fri_ref[which], jnp.float32)
        frictions.append(f)
        cohesions.append(coh_ref[which] * jnp.sqrt(1.0 - f * f))

    def table(x, carry):
        z = jnp.where(elig[x] == 1, zone[x], -1)
        c = jnp.full((rows_y, depth), 1e30, jnp.float32)
        f = jnp.zeros((rows_y, depth), jnp.float32)
        for which in range(coh_ref.shape[0]):
            hit = z == which
            c = jnp.where(hit, cohesions[which], c)
            f = jnp.where(hit, frictions[which], f)
        cc[x] = c
        cf[x] = f
        return carry

    lax.fori_loop(0, rows_x, table, 0, unroll=2)

    lane = lax.broadcasted_iota(jnp.int32, (rows_y, depth), 1)
    keep = {
        1: lane < depth - 1,
        2: lane < depth - 2,
        -1: lane >= 1,
        -2: lane >= 2,
    }

    def along_z(value, offset):
        if offset == 0:
            return value
        return jnp.where(keep[offset], pltpu.roll(value, (-offset) % depth, 1), 0.0)

    def derivative(get, forward):
        a, b, c, d = (get(1), get(0), get(2), get(-1)) if forward else (get(0), get(-1), get(1), get(-2))
        return 27.0 * (a - b) - (c - d)

    def dx(p, slot, x, forward):
        return derivative(lambda o: xb[p, slot, x + 2 + o], forward)

    def dy(p, slot, x, forward):
        return derivative(lambda o: yb[pl.ds(ybase(p, slot, x) + o, rows_y), :], forward)

    def dz(value, forward):
        return derivative(lambda o: along_z(value, o), forward)

    def put_y(p, slot, x, value):
        yb[pl.ds(pl.multiple_of(ybase(p, slot, x), 8), rows_y), :] = value

    def own_y(p, slot, x):
        return yb[pl.ds(pl.multiple_of(ybase(p, slot, x), 8), rows_y), :]

    def flow_layer(p, x):
        step = p // 2
        s = p
        scale = (time_step / 24.0) * buo[x]
        xz = xb[s, 2, x + 2]
        yz = own_y(s, 2, x)
        zz = zb[step, x]
        force_x = dx(s, 0, x, True) + dy(s, 0, x, False) + dz(xz, False)
        force_y = dx(s, 1, x, False) + dy(s, 1, x, True) + dz(yz, False)
        force_z = dx(s, 2, x, False) + dy(s, 2, x, False) + dz(zz, True)
        for slot, force in enumerate((force_x, force_y, force_z)):
            old = vel[slot, x] if step == 0 else xb[p - 1, slot, x + 2]
            new = old + scale * force
            xb[p + 1, slot, x + 2] = new
            put_y(p + 1, slot, x, new)

    def stress_layer(p, x):
        step = p // 2
        vx, vy, vz = (xb[p, slot, x + 2] for slot in range(3))
        ex = dx(p, 0, x, False)
        ey = dy(p, 1, x, False)
        ez = dz(vz, False)
        xy = dy(p, 0, x, True) + dx(p, 1, x, True)
        xz = dz(vx, True) + dx(p, 2, x, True)
        yz = dz(vy, True) + dy(p, 2, x, True)
        m = (time_step / 24.0) * mod[x]
        spread = (time_step / 24.0) * lam[x] * (ex + ey + ez)
        m2 = m + m
        s0, s3, s4 = (xb[p - 1, slot, x + 2] for slot in range(3))
        s1, s5 = own_y(p - 1, 1, x), own_y(p - 1, 2, x)
        s2 = zb[step, x]
        s0 = s0 + (spread + m2 * ex) + inj[0, x]
        s1 = s1 + (spread + m2 * ey) + inj[1, x]
        s2 = s2 + (spread + m2 * ez) + inj[2, x]
        s3 = s3 + m * xy + inj[3, x]
        s4 = s4 + m * xz + inj[4, x]
        s5 = s5 + m * yz + inj[5, x]
        pressure = (s0 + s1 + s2) * (1.0 / 3.0)
        d0, d1, d2 = s0 - pressure, s1 - pressure, s2 - pressure
        second = 0.5 * (d0 * d0 + d1 * d1 + d2 * d2) + (s3 * s3 + s4 * s4 + s5 * s5)
        strength = jnp.maximum(cc[x] - pressure * cf[x], 0.0)
        factor = jnp.minimum(1.0, strength * lax.rsqrt(jnp.maximum(second, shear_floor * shear_floor)))
        s0, s1, s2 = pressure + factor * d0, pressure + factor * d1, pressure + factor * d2
        s3, s4, s5 = factor * s3, factor * s4, factor * s5
        if p == phases - 1:
            for comp, value in enumerate((s0, s1, s2, s3, s4, s5)):
                sout[comp, x] = value
            return
        for slot, value in enumerate((s0, s3, s4)):
            xb[p + 1, slot, x + 2] = value
        for slot, value in enumerate((s3, s1, s5)):
            put_y(p + 1, slot, x, value)
        zb[step + 1, x] = s2

    stores = []

    def store(src, dst):
        copy = pltpu.make_async_copy(src, dst, store_sem.at[len(stores)])
        copy.start()
        stores.append(copy)

    waited = {5: False, 8: False, 9: False, 10: False, 11: False}

    def need(*which):
        for i in which:
            if not waited[i]:
                waited[i] = True
                loads[i].wait()

    for p in range(phases):
        if p % 2 == 0:
            need(5, 8, 9)
            layer_of = flow_layer
        else:
            need(10, 11)
            layer_of = stress_layer
        for c in order:
            if c == 0:
                take_x(p, True)
            if c == chunks - 1:
                take_x(p, False)
            take_y(p, c)

            def one(i, carry, p=p, c=c, layer_of=layer_of):
                layer_of(p, c * CH + i)
                return carry

            lax.fori_loop(0, CH, one, 0, unroll=UNROLL)
            span = pl.ds(c * CH, CH)
            if p < phases - 1:
                if c == 0:
                    send_x(p + 1, False)
                if c == chunks - 1:
                    send_x(p + 1, True)
                send_y(p + 1, c)
            else:
                store(sout.at[:, span], sout_hbm.at[:, span])
            if p == phases - 2:
                for slot in range(3):
                    store(xb.at[p + 1, slot, pl.ds(2 + c * CH, CH)], vout_hbm.at[slot, span])

    for p in range(phases):
        for there, way in ((x_hi, True), (x_lo, False)):

            @pl.when(there)
            def _():
                for slot in range(3):
                    x_copy(p, slot, way).wait_send()

        for there, way in ((y_hi, True), (y_lo, False)):

            @pl.when(there)
            def _():
                for c in range(chunks):
                    y_copy(p, c, way).wait_send()

    for copy in stores:
        copy.wait()


def on_device(nx, ny, velocity, stress, lame_first, modulus, buoyancy, zone, eligible, cohesion, friction, source_cell, source_moment):
    rows_x, rows_y, depth = zone.shape
    assert rows_y <= 8 and rows_x % CH == 0
    chunks = rows_x // CH
    phases = 2 * STEPS
    f32 = jnp.float32
    grid = (rows_x, rows_y, depth)
    any_spec = pl.BlockSpec(memory_space=pltpu.HBM)
    smem = pl.BlockSpec(memory_space=pltpu.SMEM)
    vmem = pl.BlockSpec(memory_space=pltpu.VMEM)
    return pl.pallas_call(
        functools.partial(kernel, nx, ny),
        out_shape=(jax.ShapeDtypeStruct((3,) + grid, f32), jax.ShapeDtypeStruct((6,) + grid, f32)),
        in_specs=[any_spec] * 7 + [smem, smem, vmem, vmem],
        out_specs=(any_spec, any_spec),
        scratch_shapes=[
            pltpu.VMEM((2,) + grid, f32),
            pltpu.VMEM((3,) + grid, f32),
            pltpu.VMEM(grid, f32),
            pltpu.VMEM(grid, f32),
            pltpu.VMEM(grid, f32),
            pltpu.VMEM(grid, jnp.int32),
            pltpu.VMEM(grid, jnp.int32),
            pltpu.VMEM((6,) + grid, f32),
            pltpu.VMEM(grid, f32),
            pltpu.VMEM(grid, f32),
            pltpu.VMEM((6,) + grid, f32),
            pltpu.VMEM((phases, 3, rows_x + 4, rows_y, depth), f32),
            pltpu.VMEM((phases * 3 * R * (rows_x + 1) + R, depth), f32),
            pltpu.VMEM((STEPS,) + grid, f32),
            pltpu.VMEM((phases, chunks, 5 * CH, depth), f32),
            pltpu.VMEM((phases, chunks, 5 * CH, depth), f32),
            pltpu.VMEM((phases, chunks, 5 * CH, depth), f32),
            pltpu.VMEM((phases, chunks, 5 * CH, depth), f32),
            pltpu.SemaphoreType.DMA((12,)),
            pltpu.SemaphoreType.DMA((4 * chunks,)),
            pltpu.SemaphoreType.DMA((phases, 2, 3)),
            pltpu.SemaphoreType.DMA((phases, 2, 3)),
            pltpu.SemaphoreType.DMA((phases, 2, chunks)),
            pltpu.SemaphoreType.DMA((phases, 2, chunks)),
        ],
        compiler_params=pltpu.CompilerParams(collective_id=0, has_side_effects=True),
    )(
        velocity, stress, lame_first, modulus, buoyancy, zone, eligible,
        cohesion, friction, source_cell.reshape(1, -1), source_moment,
    )


def solution(mesh):
    field = P(None, "gx", "gy", None)
    cells = P("gx", "gy", None)
    return jax.shard_map(
        functools.partial(on_device, mesh.shape["gx"], mesh.shape["gy"]),
        mesh=mesh,
        in_specs=(field, field, cells, cells, cells, cells, cells, P(), P(), P(), P()),
        out_specs=(field, field),
        check_vma=False,
    )
```

```python
import functools

import jax
import jax.numpy as jnp
from jax import lax
from jax.experimental import pallas as pl
from jax.experimental.pallas import tpu as pltpu
from jax.sharding import PartitionSpec as P

STEPS = 2
time_step = 0.1
shear_floor = 0.25
MESH = pl.DeviceIdType.MESH
CH = 8
R = 16

STRESS_X = ((0, 1, 2), (3, 2, 1), (4, 2, 1))
STRESS_Y = ((3, 2, 1), (1, 1, 2), (5, 2, 1))
FLOW_X = ((0, 2, 1), (1, 1, 2), (2, 1, 2))
FLOW_Y = ((0, 1, 2), (1, 2, 1), (2, 1, 2))
SPEC = {"s": (STRESS_X, STRESS_Y), "v": (FLOW_X, FLOW_Y)}


def kernel(
    nx,
    ny,
    vel_hbm, str_hbm, lam_hbm, mod_hbm, buo_hbm, zone_hbm, elig_hbm,
    coh_ref, fri_ref, cell_ref, moment_ref,
    vout_ref, sout_ref,
    xe, stage, vel, lam, mod, buo, zone, elig, inj, cc, cf,
    xb, yb, zb, pack_up, pack_dn, recv_up, recv_dn,
    load_sem, xsend, xrecv, ysend, yrecv,
):
    rows_x = lam.shape[0]
    rows_y = lam.shape[1]
    depth = lam.shape[2]
    chunks = rows_x // CH
    block = R * (rows_x + 1)
    phases = 2 * STEPS
    ix = lax.axis_index("gx")
    iy = lax.axis_index("gy")
    x_lo, x_hi, y_lo, y_hi = ix > 0, ix < nx - 1, iy > 0, iy < ny - 1

    barrier = pltpu.get_barrier_semaphore()
    sides = (
        (x_lo, (ix - 1, iy)),
        (x_hi, (ix + 1, iy)),
        (y_lo, (ix, iy - 1)),
        (y_hi, (ix, iy + 1)),
    )
    for there, target in sides:

        @pl.when(there)
        def _():
            pl.semaphore_signal(barrier, inc=1, device_id=target, device_id_type=MESH)

    loads = []

    def load(src, dst):
        copy = pltpu.make_async_copy(src, dst, load_sem.at[len(loads)])
        copy.start()
        loads.append(copy)

    for slot, (comp, low, high) in enumerate(STRESS_X):
        load(str_hbm.at[comp, pl.ds(rows_x - low, low)], xe.at[0, slot, pl.ds(0, low)])
        load(str_hbm.at[comp, pl.ds(0, high)], xe.at[1, slot, pl.ds(0, high)])
    edges, rest = len(loads), len(loads) + 3
    load(str_hbm.at[3], xb.at[0, 1, pl.ds(2, rows_x)])
    load(str_hbm.at[1], stage.at[0])
    load(str_hbm.at[5], stage.at[1])
    load(zone_hbm, zone)
    load(elig_hbm, elig)
    load(str_hbm.at[0], xb.at[0, 0, pl.ds(2, rows_x)])
    load(str_hbm.at[4], xb.at[0, 2, pl.ds(2, rows_x)])
    load(str_hbm.at[2], zb.at[0])
    load(vel_hbm, vel)
    load(buo_hbm, buo)
    late = len(loads)
    load(lam_hbm, lam)
    load(mod_hbm, mod)

    zero = jnp.zeros((rows_y, depth), jnp.float32)

    @pl.when(jnp.logical_not(x_lo))
    def _():
        for p in range(phases):
            for slot in range(3):
                for layer in (0, 1):
                    xb[p, slot, layer] = zero

    @pl.when(jnp.logical_not(x_hi))
    def _():
        for p in range(phases):
            for slot in range(3):
                for layer in (rows_x + 2, rows_x + 3):
                    xb[p, slot, layer] = zero

    @pl.when(jnp.logical_not(y_lo))
    def _():
        for p in range(phases):
            for c in range(chunks):
                recv_up[p, c] = jnp.zeros(recv_up.shape[2:], jnp.float32)

    @pl.when(jnp.logical_not(y_hi))
    def _():
        for p in range(phases):
            for c in range(chunks):
                recv_dn[p, c] = jnp.zeros(recv_dn.shape[2:], jnp.float32)

    def x_copy(p, slot, up):
        comp, low, high = SPEC["sv"[p % 2]][0][slot]
        if up:
            src = xe.at[0, slot, pl.ds(0, low)] if p == 0 else xb.at[p, slot, pl.ds(rows_x + 2 - low, low)]
            dst = xb.at[p, slot, pl.ds(2 - low, low)]
            target = (ix + 1, iy)
        else:
            src = xe.at[1, slot, pl.ds(0, high)] if p == 0 else xb.at[p, slot, pl.ds(2, high)]
            dst = xb.at[p, slot, pl.ds(rows_x + 2, high)]
            target = (ix - 1, iy)
        way = 0 if up else 1
        return pltpu.make_async_remote_copy(
            src_ref=src,
            dst_ref=dst,
            send_sem=xsend.at[p, way, slot],
            recv_sem=xrecv.at[p, way, slot],
            device_id=target,
            device_id_type=MESH,
        )

    def y_layers(p):
        spec = SPEC["sv"[p % 2]][1]
        up = [(slot, rows_y - low + i, i - low) for slot, (_, low, _) in enumerate(spec) for i in range(low)]
        dn = [(slot, i, rows_y + i) for slot, (_, _, high) in enumerate(spec) for i in range(high)]
        return up, dn

    def y_copy(p, c, up):
        rows = CH * len(y_layers(p)[0 if up else 1])
        packed, recv = (pack_up, recv_up) if up else (pack_dn, recv_dn)
        way = 0 if up else 1
        return pltpu.make_async_remote_copy(
            src_ref=packed.at[p, c, pl.ds(0, rows)],
            dst_ref=recv.at[p, c, pl.ds(0, rows)],
            send_sem=ysend.at[p, way, c],
            recv_sem=yrecv.at[p, way, c],
            device_id=(ix, iy + 1) if up else (ix, iy - 1),
            device_id_type=MESH,
        )

    def send_x(p, up):
        @pl.when(x_hi if up else x_lo)
        def _():
            for slot in range(3):
                x_copy(p, slot, up).start()

    def take_x(p, up):
        @pl.when(x_lo if up else x_hi)
        def _():
            for slot in range(3):
                x_copy(p, slot, up).wait_recv()

    def ybase(p, slot, x):
        return (p * 3 + slot) * block + R * (x + 1)

    def send_y(p, c):
        up, dn = y_layers(p)
        for layers, packed in ((up, pack_up), (dn, pack_dn)):
            for i, (slot, row, _) in enumerate(layers):
                start = ybase(p, slot, c * CH) + row
                packed[p, c, pl.ds(i * CH, CH), :] = yb[pl.ds(start, CH, stride=R), :]
        for there, way in ((y_hi, True), (y_lo, False)):

            @pl.when(there)
            def _():
                y_copy(p, c, way).start()

    def take_y(p, c):
        for there, way in ((y_lo, True), (y_hi, False)):

            @pl.when(there)
            def _():
                y_copy(p, c, way).wait_recv()

        up, dn = y_layers(p)
        for layers, recv in ((up, recv_up), (dn, recv_dn)):
            for i, (slot, _, row) in enumerate(layers):
                start = ybase(p, slot, c * CH) + row
                yb[pl.ds(start, CH, stride=R), :] = recv[p, c, pl.ds(i * CH, CH), :]

    order = [0] + ([chunks - 1] if chunks > 1 else []) + list(range(1, chunks - 1))

    for copy in loads[:edges]:
        copy.wait()

    def fill_y(c):
        def fill(i, carry):
            x = c * CH + i
            for slot, source in enumerate((None, 0, 1)):
                value = xb[0, 1, x + 2] if source is None else stage[source, x]
                yb[pl.ds(pl.multiple_of(ybase(0, slot, x), 8), rows_y), :] = value
            return carry

        lax.fori_loop(0, CH, fill, 0, unroll=True)

    heard = sum(there.astype(jnp.int32) for there, _ in sides)
    pl.semaphore_wait(barrier, heard)
    send_x(0, True)
    send_x(0, False)
    for copy in loads[edges:rest]:
        copy.wait()
    for c in order:
        fill_y(c)
        send_y(0, c)

    cell = cell_ref[...]
    bits = depth.bit_length() - 1
    assert depth == 1 << bits
    plane_row = cell >> bits
    cell_z = cell & (depth - 1)
    row = lax.broadcasted_iota(jnp.int32, (rows_x * rows_y, cell.shape[1]), 0)
    row_bits = rows_y.bit_length() - 1
    assert rows_y == 1 << row_bits
    row = (ix * rows_x + (row >> row_bits)) * (ny * rows_y) + iy * rows_y + (row & (rows_y - 1))
    match = row == plane_row
    at_z = (lax.broadcasted_iota(jnp.int32, (depth, cell.shape[1]), 0) == cell_z).astype(jnp.float32)
    for comp in range(6):
        moment = time_step * moment_ref[pl.ds(comp, 1), :]
        value = lax.dot_general(
            jnp.where(match, moment, 0.0),
            at_z,
            (((1,), (1,)), ((), ())),
            precision=lax.Precision.HIGHEST,
            preferred_element_type=jnp.float32,
        )
        inj[comp] = value.reshape(rows_x, rows_y, depth)

    for copy in loads[rest : rest + 2]:
        copy.wait()
    frictions, cohesions = [], []
    for which in range(coh_ref.shape[0]):
        f = jnp.full((rows_y, depth), fri_ref[which], jnp.float32)
        frictions.append(f)
        cohesions.append(coh_ref[which] * jnp.sqrt(1.0 - f * f))

    def table(x, carry):
        z = jnp.where(elig[x] == 1, zone[x], -1)
        c = jnp.full((rows_y, depth), 1e30, jnp.float32)
        f = jnp.zeros((rows_y, depth), jnp.float32)
        for which in range(coh_ref.shape[0]):
            hit = z == which
            c = jnp.where(hit, cohesions[which], c)
            f = jnp.where(hit, frictions[which], f)
        cc[x] = c
        cf[x] = f
        return carry

    lax.fori_loop(0, rows_x, table, 0, unroll=2)

    lane = lax.broadcasted_iota(jnp.int32, (rows_y, depth), 1)
    keep = {
        1: lane < depth - 1,
        2: lane < depth - 2,
        -1: lane >= 1,
        -2: lane >= 2,
    }

    def along_z(value, offset):
        if offset == 0:
            return value
        return jnp.where(keep[offset], pltpu.roll(value, (-offset) % depth, 1), 0.0)

    def derivative(get, forward):
        a, b, c, d = (get(1), get(0), get(2), get(-1)) if forward else (get(0), get(-1), get(1), get(-2))
        return 27.0 * (a - b) - (c - d)

    def dx(p, slot, x, forward):
        return derivative(lambda o: xb[p, slot, x + 2 + o], forward)

    def dy(p, slot, x, forward):
        return derivative(lambda o: yb[pl.ds(ybase(p, slot, x) + o, rows_y), :], forward)

    def dz(value, forward):
        return derivative(lambda o: along_z(value, o), forward)

    def put_y(p, slot, x, value):
        yb[pl.ds(pl.multiple_of(ybase(p, slot, x), 8), rows_y), :] = value

    def own_y(p, slot, x):
        return yb[pl.ds(pl.multiple_of(ybase(p, slot, x), 8), rows_y), :]

    def flow_layer(p, x):
        step = p // 2
        s = p
        scale = (time_step / 24.0) * buo[x]
        xz = xb[s, 2, x + 2]
        yz = own_y(s, 2, x)
        zz = zb[step, x]
        force_x = dx(s, 0, x, True) + dy(s, 0, x, False) + dz(xz, False)
        force_y = dx(s, 1, x, False) + dy(s, 1, x, True) + dz(yz, False)
        force_z = dx(s, 2, x, False) + dy(s, 2, x, False) + dz(zz, True)
        for slot, force in enumerate((force_x, force_y, force_z)):
            old = vel[slot, x] if step == 0 else xb[p - 1, slot, x + 2]
            new = old + scale * force
            xb[p + 1, slot, x + 2] = new
            put_y(p + 1, slot, x, new)
            if p == phases - 2:
                vout_ref[slot, x] = new

    def stress_layer(p, x):
        step = p // 2
        vx, vy, vz = (xb[p, slot, x + 2] for slot in range(3))
        ex = dx(p, 0, x, False)
        ey = dy(p, 1, x, False)
        ez = dz(vz, False)
        xy = dy(p, 0, x, True) + dx(p, 1, x, True)
        xz = dz(vx, True) + dx(p, 2, x, True)
        yz = dz(vy, True) + dy(p, 2, x, True)
        m = (time_step / 24.0) * mod[x]
        spread = (time_step / 24.0) * lam[x] * (ex + ey + ez)
        m2 = m + m
        s0, s3, s4 = (xb[p - 1, slot, x + 2] for slot in range(3))
        s1, s5 = own_y(p - 1, 1, x), own_y(p - 1, 2, x)
        s2 = zb[step, x]
        s0 = s0 + (spread + m2 * ex) + inj[0, x]
        s1 = s1 + (spread + m2 * ey) + inj[1, x]
        s2 = s2 + (spread + m2 * ez) + inj[2, x]
        s3 = s3 + m * xy + inj[3, x]
        s4 = s4 + m * xz + inj[4, x]
        s5 = s5 + m * yz + inj[5, x]
        pressure = (s0 + s1 + s2) * (1.0 / 3.0)
        d0, d1, d2 = s0 - pressure, s1 - pressure, s2 - pressure
        second = 0.5 * (d0 * d0 + d1 * d1 + d2 * d2) + (s3 * s3 + s4 * s4 + s5 * s5)
        strength = jnp.maximum(cc[x] - pressure * cf[x], 0.0)
        factor = jnp.minimum(1.0, strength * lax.rsqrt(jnp.maximum(second, shear_floor * shear_floor)))
        s0, s1, s2 = pressure + factor * d0, pressure + factor * d1, pressure + factor * d2
        s3, s4, s5 = factor * s3, factor * s4, factor * s5
        if p == phases - 1:
            for comp, value in enumerate((s0, s1, s2, s3, s4, s5)):
                sout_ref[comp, x] = value
            return
        for slot, value in enumerate((s0, s3, s4)):
            xb[p + 1, slot, x + 2] = value
        for slot, value in enumerate((s3, s1, s5)):
            put_y(p + 1, slot, x, value)
        zb[step + 1, x] = s2

    for p in range(phases):
        layer_of = flow_layer if p % 2 == 0 else stress_layer
        if p == 0:
            for copy in loads[rest + 2 : late]:
                copy.wait()
        elif p == 1:
            for copy in loads[late:]:
                copy.wait()
        for c in order:
            if c == 0:
                take_x(p, True)
            if c == chunks - 1:
                take_x(p, False)
            take_y(p, c)

            def one(i, carry, p=p, c=c, layer_of=layer_of):
                layer_of(p, c * CH + i)
                return carry

            lax.fori_loop(0, CH, one, 0, unroll=True)
            if p < phases - 1:
                if c == 0:
                    send_x(p + 1, False)
                if c == chunks - 1:
                    send_x(p + 1, True)
                send_y(p + 1, c)

    for p in range(phases):
        for there, way in ((x_hi, True), (x_lo, False)):

            @pl.when(there)
            def _():
                for slot in range(3):
                    x_copy(p, slot, way).wait_send()

        for there, way in ((y_hi, True), (y_lo, False)):

            @pl.when(there)
            def _():
                for c in range(chunks):
                    y_copy(p, c, way).wait_send()


def on_device(nx, ny, velocity, stress, lame_first, modulus, buoyancy, zone, eligible, cohesion, friction, source_cell, source_moment):
    rows_x, rows_y, depth = zone.shape
    assert rows_y <= 8 and rows_x % CH == 0
    chunks = rows_x // CH
    phases = 2 * STEPS
    f32 = jnp.float32
    grid = (rows_x, rows_y, depth)
    any_spec = pl.BlockSpec(memory_space=pltpu.HBM)
    smem = pl.BlockSpec(memory_space=pltpu.SMEM)
    vmem = pl.BlockSpec(memory_space=pltpu.VMEM)
    return pl.pallas_call(
        functools.partial(kernel, nx, ny),
        out_shape=(pltpu.VMEM((3,) + grid, f32), pltpu.VMEM((6,) + grid, f32)),
        in_specs=[any_spec] * 7 + [smem, smem, vmem, vmem],
        out_specs=(vmem, vmem),
        scratch_shapes=[
            pltpu.VMEM((2, 3, 2, rows_y, depth), f32),
            pltpu.VMEM((2,) + grid, f32),
            pltpu.VMEM((3,) + grid, f32),
            pltpu.VMEM(grid, f32),
            pltpu.VMEM(grid, f32),
            pltpu.VMEM(grid, f32),
            pltpu.VMEM(grid, jnp.int32),
            pltpu.VMEM(grid, jnp.int32),
            pltpu.VMEM((6,) + grid, f32),
            pltpu.VMEM(grid, f32),
            pltpu.VMEM(grid, f32),
            pltpu.VMEM((phases, 3, rows_x + 4, rows_y, depth), f32),
            pltpu.VMEM((phases * 3 * R * (rows_x + 1) + R, depth), f32),
            pltpu.VMEM((STEPS,) + grid, f32),
            pltpu.VMEM((phases, chunks, 5 * CH, depth), f32),
            pltpu.VMEM((phases, chunks, 5 * CH, depth), f32),
            pltpu.VMEM((phases, chunks, 5 * CH, depth), f32),
            pltpu.VMEM((phases, chunks, 5 * CH, depth), f32),
            pltpu.SemaphoreType.DMA((18,)),
            pltpu.SemaphoreType.DMA((phases, 2, 3)),
            pltpu.SemaphoreType.DMA((phases, 2, 3)),
            pltpu.SemaphoreType.DMA((phases, 2, chunks)),
            pltpu.SemaphoreType.DMA((phases, 2, chunks)),
        ],
        compiler_params=pltpu.CompilerParams(collective_id=0, has_side_effects=True),
    )(
        velocity, stress, lame_first, modulus, buoyancy, zone, eligible,
        cohesion, friction, source_cell.reshape(1, -1), source_moment,
    )


def solution(mesh):
    field = P(None, "gx", "gy", None)
    cells = P("gx", "gy", None)
    return jax.shard_map(
        functools.partial(on_device, mesh.shape["gx"], mesh.shape["gy"]),
        mesh=mesh,
        in_specs=(field, field, cells, cells, cells, cells, cells, P(), P(), P(), P()),
        out_specs=(field, field),
        check_vma=False,
    )
```
